32 devices in a mesh: samp: 8 (over z, core), var: 4 (over y, x).
Axes of the slice: x: 2, y: 2, z: 4, core: 2. Of those that a mesh axis runs over, the one named last changes fastest.
Arguments:
- hap_words: int32 [2, 512, 512], P(None, 'samp', 'var'), may hold values from 0 to 1073741823
- total_counts: int32 [15360, 8192], P('samp', 'var'), may hold values from 0 to 4999
- allele_one: int32 [15360, 8192], P('samp', 'var'), may hold values from 0 to 299
- allele_two: int32 [15360, 8192], P('samp', 'var'), may hold values from 0 to 299
Outputs:
- z_total: float32 [512, 8192], P('samp', 'var')
- z_allelic: float32 [512, 8192], P('samp', 'var')
The draws below stay inside these ranges and needn't reach their ends.
Inputs may be any that keep to these rules, and one draw needn't show every extreme that they name: Bit k, for k below 30, of hap_words[c, j, v] is haplotype c of sample 30 * j + k at variant v; higher bits are zero.
All inputs are finite; a program needn't handle non-finite values.
Results may differ from the reference program's by a relative error of at most 0.0003.
The reference program's roundings to bfloat16 on the way count: a program that leaves them out, or rounds other values in their place, can miss the bound.
Values sent between devices are 32-bit elements; how exact they have to be, the bound alone decides.
A program may use at most 192 MiB of HBM per device.

```python
import jax
import jax.numpy as jnp
from jax import lax

BITS = 30
GENES = 8192
SWORDS = 512
SAMPLES = 15360
VARIANTS = 512


def with_ends(array, own_key, low, high):
    longest = array.shape.index(max(array.shape))
    spots = []
    for shift in (0, 1):
        where = [jax.random.randint(jax.random.fold_in(own_key, axis), (), 0, length) for axis, length in enumerate(array.shape)]
        where[longest] = (where[longest] + shift) % array.shape[longest]
        spots.append(tuple(where))
    return array.at[spots[0]].set(low).at[spots[1]].set(high)


def setup_inputs(seed: int = 0) -> dict:
    seeds = jax.random.split(jax.random.key(seed), 5)
    hap_words = with_ends(jax.random.randint(seeds[0], (2, SWORDS, VARIANTS), 0, 2 ** BITS), jax.random.fold_in(seeds[0], 1), 0, (2 ** BITS) - 1).astype(jnp.int32)
    total_counts = with_ends(jax.random.randint(seeds[1], (SAMPLES, GENES), 0, 5000), jax.random.fold_in(seeds[1], 1), 0, 4999).astype(jnp.int32)
    allele_one = with_ends(jax.random.randint(seeds[2], (SAMPLES, GENES), 0, 300), jax.random.fold_in(seeds[2], 1), 0, 299).astype(jnp.int32)
    allele_two = with_ends(jax.random.randint(seeds[3], (SAMPLES, GENES), 0, 300), jax.random.fold_in(seeds[3], 1), 0, 299).astype(jnp.int32)
    return dict(hap_words=hap_words, total_counts=total_counts, allele_one=allele_one, allele_two=allele_two)


def unpack(packed):
    shifts = jnp.arange(BITS, dtype=jnp.int32)
    bit_table = jnp.bitwise_and(jnp.right_shift(packed[:, :, None, :], shifts[None, None, :, None]), 1)
    return bit_table.reshape(2, packed.shape[1] * BITS, packed.shape[2])

def features(total_part, one_part, two_part):
    log_total = jnp.log1p(total_part.astype(jnp.float32))
    one_plus = one_part.astype(jnp.float32) + 1.0
    two_plus = two_part.astype(jnp.float32) + 1.0
    log_ratio = jnp.log(one_plus / two_plus)
    weight = 1.0 / (1.0 / one_plus + 1.0 / two_plus)
    return (log_total, (weight * log_ratio).astype(jnp.bfloat16), weight.astype(jnp.bfloat16))

def finish(cross_total, cross_allelic, het_weight, dos_sum, dos_sq, gene_sum, gene_sq, sample_count):
    dosage_var = dos_sq - dos_sum * dos_sum / sample_count
    gene_var = gene_sq - gene_sum * gene_sum / sample_count
    covariance = cross_total - dos_sum[:, None] * gene_sum[None, :] / sample_count
    z_total = jnp.sqrt(sample_count) * covariance / jnp.sqrt((dosage_var[:, None] + 1.0) * (gene_var[None, :] + 1.0))
    z_allelic = cross_allelic / jnp.sqrt(het_weight + 1.0)
    return (z_total, z_allelic)

def reference(hap_words, total_counts, allele_one, allele_two):
    bit_table = unpack(hap_words)
    dosage = bit_table[0] + bit_table[1] - 1
    phase_diff = bit_table[0] - bit_table[1]
    dosage_f = dosage.astype(jnp.float32)
    dos_sum = lax.optimization_barrier(jnp.sum(dosage_f, axis=0))
    dos_sq = lax.optimization_barrier(jnp.sum(dosage_f * dosage_f, axis=0))
    dosage_b = dosage.astype(jnp.bfloat16)
    phase_b = phase_diff.astype(jnp.bfloat16)
    phase_sq_b = (phase_diff * phase_diff).astype(jnp.bfloat16)
    sample_count = jnp.float32(hap_words.shape[1] * BITS)
    block_width = GENES // 8

    def one_block(block_index):
        first_col = (block_index * block_width).astype(jnp.int32)
        total_part = lax.dynamic_slice_in_dim(total_counts, first_col, block_width, 1)
        one_part = lax.dynamic_slice_in_dim(allele_one, first_col, block_width, 1)
        two_part = lax.dynamic_slice_in_dim(allele_two, first_col, block_width, 1)
        log_total, weighted_b, weight_b = features(total_part, one_part, two_part)
        cross_total = jnp.dot(dosage_b.T, log_total.astype(jnp.bfloat16), preferred_element_type=jnp.float32)
        cross_allelic = jnp.dot(phase_b.T, weighted_b, preferred_element_type=jnp.float32)
        het_weight = jnp.dot(phase_sq_b.T, weight_b, preferred_element_type=jnp.float32)
        gene_sum = lax.optimization_barrier(jnp.sum(log_total, axis=0))
        gene_sq = lax.optimization_barrier(jnp.sum(log_total * log_total, axis=0))
        return finish(cross_total, cross_allelic, het_weight, dos_sum, dos_sq, gene_sum, gene_sq, sample_count)
    total_blocks, allelic_blocks = lax.map(one_block, jnp.arange(8, dtype=jnp.int32))
    variants = hap_words.shape[2]
    z_total = jnp.moveaxis(total_blocks, 0, 1).reshape(variants, GENES)
    z_allelic = jnp.moveaxis(allelic_blocks, 0, 1).reshape(variants, GENES)
    return (z_total, z_allelic)
```

```python
import jax
import jax.numpy as jnp
from jax import lax
from jax.sharding import PartitionSpec as P

BITS = 30


def unpack(packed):
    shifts = jnp.arange(BITS, dtype=jnp.int32)
    bit_table = jnp.bitwise_and(
        jnp.right_shift(packed[:, :, None, :], shifts[None, None, :, None]), 1
    )
    return bit_table.reshape(2, packed.shape[1] * BITS, packed.shape[2])


def features(total_part, one_part, two_part):
    log_total = jnp.log1p(total_part.astype(jnp.float32))
    one_plus = one_part.astype(jnp.float32) + 1.0
    two_plus = two_part.astype(jnp.float32) + 1.0
    log_ratio = jnp.log(one_plus / two_plus)
    weight = 1.0 / (1.0 / one_plus + 1.0 / two_plus)
    return (log_total, (weight * log_ratio).astype(jnp.bfloat16), weight.astype(jnp.bfloat16))


def finish(pair_sums, dos_margin, gene_margin, sample_count):
    dos_sum, dos_sq = (dos_margin[0], dos_margin[1])
    gene_sum, gene_sq = (gene_margin[0], gene_margin[1])
    dosage_var = dos_sq - dos_sum * dos_sum / sample_count
    gene_var = gene_sq - gene_sum * gene_sum / sample_count
    covariance = pair_sums[0] - dos_sum[:, None] * gene_sum[None, :] / sample_count
    z_total = (
        jnp.sqrt(sample_count)
        * covariance
        / jnp.sqrt((dosage_var[:, None] + 1.0) * (gene_var[None, :] + 1.0))
    )
    z_allelic = pair_sums[1] / jnp.sqrt(pair_sums[2] + 1.0)
    return (z_total, z_allelic)


def gather_words(hap_words):
    size = lax.axis_size("var")
    here = lax.axis_index("var")
    blocks = [hap_words]
    for shift in range(1, size):
        blocks.append(
            lax.ppermute(hap_words, "var", [((i + shift) % size, i) for i in range(size)])
        )
    placed = []
    for owner in range(size):
        steps = lax.rem(owner - here + size, size)
        block = blocks[0]
        for shift in range(1, size):
            block = jnp.where(steps == shift, blocks[shift], block)
        placed.append(block)
    return jnp.concatenate(placed, axis=2)


def dosage_table(packed):
    bits = unpack(packed)
    dosage_b = (bits[0] + bits[1] - 1).astype(jnp.bfloat16)
    margin = jnp.stack(
        [
            jnp.sum(dosage_b, axis=0, dtype=jnp.float32),
            jnp.sum(dosage_b * dosage_b, axis=0, dtype=jnp.float32),
        ]
    )
    return (dosage_b, margin)


def phase_tables(packed):
    bits = unpack(packed)
    phase = bits[0] - bits[1]
    return (phase.astype(jnp.bfloat16), (phase * phase).astype(jnp.bfloat16))


def pair_sum(table, feature):
    return jnp.einsum("sv,sg->vg", table, feature, preferred_element_type=jnp.float32)


def per_device(hap_words, total_counts, allele_one, allele_two):
    groups = lax.axis_size("samp")
    me = lax.axis_index("samp")
    core = lax.rem(me, 2)
    swap = [(i, i ^ 1) for i in range(groups)]
    halves = [list(range(c, groups, 2)) for c in (0, 1)]

    def scattered(chip_sum):
        return lax.psum_scatter(
            chip_sum, "samp", scatter_dimension=0, axis_index_groups=halves, tiled=True
        )

    def chip_sums(sent_table, kept_table, feature):
        partner = lax.ppermute(pair_sum(sent_table, feature), "samp", swap)
        return partner + lax.optimization_barrier(pair_sum(kept_table, feature))

    words = gather_words(hap_words)
    log_total = jnp.log1p(total_counts.astype(jnp.float32))
    gene_margin = jnp.stack([jnp.sum(log_total, axis=0), jnp.sum(log_total * log_total, axis=0)])
    total_b = log_total.astype(jnp.bfloat16)
    total_b, gene_margin = lax.optimization_barrier((total_b, gene_margin))

    width = words.shape[2] // groups
    split = words.reshape(2, words.shape[1], groups // 2, 2, width)
    flat = (2, words.shape[1], groups // 2 * width)
    low, high = (split[:, :, :, 0].reshape(flat), split[:, :, :, 1].reshape(flat))
    sent_words = jnp.where(core == 0, high, low)
    kept_words = jnp.where(core == 0, low, high)
    sent_dos, sent_margin = dosage_table(sent_words)
    kept_dos, kept_margin = dosage_table(kept_words)

    sent_total = pair_sum(sent_dos, total_b)
    kept_total = lax.optimization_barrier(pair_sum(kept_dos, total_b))
    chip_total = lax.ppermute(sent_total, "samp", swap) + kept_total
    chip_total, allele_one, allele_two, sent_words, kept_words = lax.optimization_barrier(
        (chip_total, allele_one, allele_two, sent_words, kept_words)
    )
    own_total = scattered(chip_total)
    sent_phase, sent_sq = phase_tables(sent_words)
    kept_phase, kept_sq = phase_tables(kept_words)

    _, weighted_b, weight_b = features(total_counts, allele_one, allele_two)
    weighted_b, weight_b = lax.optimization_barrier((weighted_b, weight_b))
    own_allelic = scattered(chip_sums(sent_phase, kept_phase, weighted_b))
    own_het = scattered(chip_sums(sent_sq, kept_sq, weight_b))

    parts = (2, groups // 2, width)
    even = jnp.where(core == 0, kept_margin, sent_margin).reshape(parts)
    odd = jnp.where(core == 0, sent_margin, kept_margin).reshape(parts)
    dos_margin = jnp.stack([even, odd], axis=2).reshape(2, groups * width)
    margins = jnp.concatenate([gene_margin, dos_margin], axis=1)
    margins, own_total = lax.optimization_barrier((margins, own_total))
    margins = lax.psum(margins, "samp")
    genes = gene_margin.shape[1]
    own_dos = lax.dynamic_slice_in_dim(margins, genes + me * width, width, axis=1)
    sample_count = jnp.float32(hap_words.shape[1] * BITS * groups)
    return finish(
        (own_total, own_allelic, own_het), own_dos, margins[:, :genes], sample_count
    )


def solution(mesh):
    in_specs = (P(None, "samp", "var"), P("samp", "var"), P("samp", "var"), P("samp", "var"))
    out_specs = (P("samp", "var"), P("samp", "var"))
    return jax.shard_map(
        per_device, mesh=mesh, in_specs=in_specs, out_specs=out_specs, check_vma=False
    )
```
